16 devices in a mesh: rep: 2 (over y, z), dp: 8 (over x, core).
Axes of the slice: x: 4, y: 2, z: 1, core: 2. Of those that a mesh axis runs over, the one named last changes fastest.
The devices are a block of a 4x4x8 slice.
Arguments:
- x: bfloat16 [16, 2048, 1024], P(('rep', 'dp')), parts along dimension 0
- dy: bfloat16 [16, 2048, 1024], P(('rep', 'dp')), parts along dimension 0
- w_gate: bfloat16 [2, 1024, 4096], P(None, 'dp')
- w_up: bfloat16 [2, 1024, 4096], P(None, 'dp')
- w_down: bfloat16 [2, 4096, 1024], P(None, 'dp')
- m_w_gate: float32 [2, 1024, 4096], P(None, 'dp')
- m_w_up: float32 [2, 1024, 4096], P(None, 'dp')
- m_w_down: float32 [2, 4096, 1024], P(None, 'dp')
- v_w_gate: float32 [2, 1024, 4096], P(None, 'dp')
- v_w_up: float32 [2, 1024, 4096], P(None, 'dp')
- v_w_down: float32 [2, 4096, 1024], P(None, 'dp')
Outputs:
- output 1: bfloat16 [4, 1024, 4096], P('rep', 'dp'), parts along dimension 0
- output 2: bfloat16 [4, 1024, 4096], P('rep', 'dp'), parts along dimension 0
- output 3: bfloat16 [4, 4096, 1024], P('rep', 'dp'), parts along dimension 0
- output 4: float32 [4, 1024, 4096], P('rep', 'dp'), parts along dimension 0
- output 5: float32 [4, 1024, 4096], P('rep', 'dp'), parts along dimension 0
- output 6: float32 [4, 4096, 1024], P('rep', 'dp'), parts along dimension 0
- output 7: float32 [4, 1024, 4096], P('rep', 'dp'), parts along dimension 0
- output 8: float32 [4, 1024, 4096], P('rep', 'dp'), parts along dimension 0
- output 9: float32 [4, 4096, 1024], P('rep', 'dp'), parts along dimension 0
There are 2 independent parts. The reference program is written for one: setup_inputs(seed, part) draws one part's arguments, and reference() takes and returns one part's arrays. A program takes and returns all parts, laid end to end along the dimension named above; an argument that names none is the same for every part.
All inputs are finite; a program needn't handle non-finite values.
Results may differ from the reference program's by a relative error of at most 0.022.
Values are sent between devices in bfloat16 or wider.
A program may use at most 768 MiB of HBM per device.

```python
import jax
import jax.numpy as jnp
from jax import lax

SEQUENCES = 8
TOKENS = 2048
D = 1024
FF = 4096
LAYERS = 2
NAMES = ("w_gate", "w_up", "w_down")
SHAPES = {"w_gate": (LAYERS, D, FF), "w_up": (LAYERS, D, FF), "w_down": (LAYERS, FF, D)}


def bump(key, n, height):
    away = (jnp.arange(n, dtype=jnp.int32) - jax.random.randint(key, (), 0, n, jnp.int32)) % n
    return jnp.where(away < n // 8, height, 1.0)


def together(key, own, strength):
    shared = jax.random.normal(key, own.shape[1:], jnp.float32)
    return (own + strength * shared) * lax.rsqrt(1 + strength * strength)


def setup_inputs(seed: int = 0, part: int = 0) -> dict:
    kx, kdy, ka, kb, kz, kf, kh, kl, *keys = jax.random.split(jax.random.key(seed), 8 + 3 * len(NAMES))
    kx, kdy, ka, kb = (jax.random.fold_in(k, part) for k in (kx, kdy, ka, kb))
    kw, km, kv = (keys[i::3] for i in range(3))
    shape = (SEQUENCES, TOKENS, D)
    much_x, much_dy = jax.random.uniform(kz, (2,), jnp.float32, 0.0, 1.0)
    loud = 2.0 ** jax.random.uniform(jax.random.fold_in(kz, 1), (), jnp.float32, -1.0, 2.0)
    layers = 2.0 ** jax.random.uniform(kl, (LAYERS, 1, 1), jnp.float32, -1.0, 1.0)
    x = together(ka, jax.random.normal(kx, shape, jnp.float32), much_x) * bump(kf, D, 4.0)
    dy = together(kb, jax.random.normal(kdy, shape, jnp.float32), much_dy)
    drawn = {"x": x.astype(jnp.bfloat16), "dy": (loud * dy * (SEQUENCES * TOKENS) ** -0.5).astype(jnp.bfloat16)}
    for key, name in zip(kw, NAMES, strict=True):
        w = jax.random.normal(key, SHAPES[name], jnp.float32) * SHAPES[name][1] ** -0.5
        drawn[name] = (w * {"w_gate": 1.0, "w_up": bump(kh, FF, 4.0), "w_down": layers}[name]).astype(jnp.bfloat16)
    for key, name in zip(km, NAMES, strict=True):
        drawn[f"m_{name}"] = 0.1 * jax.random.normal(key, SHAPES[name], jnp.float32)
    for key, name in zip(kv, NAMES, strict=True):
        drawn[f"v_{name}"] = jax.random.uniform(key, SHAPES[name], jnp.float32, 0.005, 0.015)
    return drawn


def matmul(a, w):
    return jnp.dot(a, w, preferred_element_type=jnp.float32).astype(jnp.bfloat16)


def normed(h):
    wide = h.astype(jnp.float32)
    scale = lax.rsqrt(jnp.mean(wide**2, -1, keepdims=True) + 1e-6)
    return (wide * scale).astype(jnp.bfloat16)


def layer(h, w):
    a = normed(h)
    gate = jnp.dot(a, w["w_gate"], preferred_element_type=jnp.float32)
    up = jnp.dot(a, w["w_up"], preferred_element_type=jnp.float32)
    return h + matmul((jax.nn.silu(gate) * up).astype(jnp.bfloat16), w["w_down"])


def adamw(w, m, v, g):
    m = 0.9 * m + 0.1 * g
    v = 0.95 * v + 0.05 * g * g
    step = m * lax.rsqrt(v + 1e-8) + 0.1 * w
    return (w - 0.02 * step).astype(jnp.bfloat16), m, v


def stack(weights, h):
    return lax.scan(lambda h, w: (layer(h, w), None), h, weights)[0]


def reference(x, dy, w_gate, w_up, w_down, m_w_gate, m_w_up, m_w_down, v_w_gate, v_w_up, v_w_down):
    weights = dict(zip(NAMES, (w_gate, w_up, w_down), strict=True))

    def take(so_far, sequence):
        h, by_y = sequence
        _, back = jax.vjp(lambda w: stack(w, h), weights)
        return jax.tree.map(lambda total, term: total + term.astype(jnp.float32), so_far, back(by_y)[0]), None

    none_yet = {name: jnp.zeros(w.shape, jnp.float32) for name, w in weights.items()}
    by_weights, _ = lax.scan(take, none_yet, (x, dy))
    gradients = [by_weights[name].astype(jnp.bfloat16).astype(jnp.float32) for name in NAMES]
    new = [
        adamw(w.astype(jnp.float32), m, v, g)
        for w, m, v, g in zip((w_gate, w_up, w_down), (m_w_gate, m_w_up, m_w_down), (v_w_gate, v_w_up, v_w_down), gradients, strict=True)
    ]
    return tuple(one[which] for which in range(3) for one in new)
```

```python
import functools

import jax
import jax.numpy as jnp
from jax import lax
from jax.experimental import pallas as pl
from jax.experimental.pallas import tpu as pltpu
from jax.sharding import PartitionSpec as P

NAMES = ("w_gate", "w_up", "w_down")
MESH = pl.DeviceIdType.MESH
F32, BF16 = jnp.float32, jnp.bfloat16
R = 128
CH = 512
BM = 512
EPS = 1e-6
COMM = True
COMPUTE = True


def nn(a, b):
    return jnp.dot(a, b, preferred_element_type=F32)


def nt(a, b):
    return lax.dot_general(a, b, (((1,), (1,)), ((), ())), preferred_element_type=F32)


def tn(a, b):
    return lax.dot_general(a, b, (((0,), (0,)), ((), ())), preferred_element_type=F32)


def kernel(
    chips, layers, groups, x, dy, own, gout, agb, part, save,
    A0, A1, H, DY, ACC, WGU, WD, HID, DG, DU, ST, DWS, DWD, R0, PB, C, F, Q, G,
    in_sem, ag_send, ag_relay, ag_l, ag_r, ag_o, ag_p, ag_loc, w_sem, st_sem, dw_sem,
    s0, r0, lp, ss, rc, rf, g_sem, credit0, credit_l, credit_r,
):
    tokens, d = x.shape
    per_layer = 3 * groups
    packets = layers * per_layer
    chunks = 2 * groups
    me = lax.axis_index("dp")
    X, c = me // 2, lax.rem(me, 2)
    XR, XL, XO = lax.rem(X + 1, chips), lax.rem(X + chips - 1, chips), lax.rem(X + 2, chips)
    right, left, partner = {"dp": 2 * XR + c}, {"dp": 2 * XL + c}, {"dp": 2 * X + 1 - c}

    def remote(src, dst, send, recv, to):
        return pltpu.make_async_remote_copy(src_ref=src, dst_ref=dst, send_sem=send, recv_sem=recv, device_id=to, device_id_type=MESH)

    local = pltpu.make_async_copy

    def when(cond):
        if isinstance(cond, bool):
            return (lambda f: f()) if cond else (lambda f: None)
        return pl.when(cond)

    def e0(p):
        for to, sem in ((right, ag_l), (left, ag_r), (partner, ag_p)):
            remote(own.at[p], agb.at[p, X, c], ag_send.at[p], sem.at[p], to).start()
        local(own.at[p], agb.at[p, X, c], ag_loc.at[p]).start()

    def e1(p):
        remote(agb.at[p, XL, c], agb.at[p, XL, c], ag_send.at[p], ag_l.at[p], right).wait_recv()
        remote(agb.at[p, XL, c, 0], agb.at[p, XL, c, 0], ag_send.at[p], ag_o.at[p], right).start()
        remote(agb.at[p, XL, c], agb.at[p, XL, c], ag_relay.at[p], ag_p.at[p], partner).start()
        remote(agb.at[p, XR, c], agb.at[p, XR, c], ag_send.at[p], ag_r.at[p], left).wait_recv()
        remote(agb.at[p, XR, c, 1], agb.at[p, XR, c, 1], ag_send.at[p], ag_o.at[p], left).start()
        remote(agb.at[p, XR, c], agb.at[p, XR, c], ag_relay.at[p], ag_p.at[p], partner).start()

    def e2(p):
        remote(agb.at[p, XO, c], agb.at[p, XO, c], ag_relay.at[p], ag_o.at[p], partner).wait_recv()
        remote(agb.at[p, XO, c], agb.at[p, XO, c], ag_relay.at[p], ag_p.at[p], partner).start()

    def ready(p):
        if not COMM:
            return
        everyone = agb.at[p, :, 1 - c]
        remote(everyone, everyone, ag_relay.at[p], ag_p.at[p], partner).wait_recv()
        local(own.at[p], agb.at[p, X, c], ag_loc.at[p]).wait()

    def ag_tick(a):
        if not COMM:
            return
        when(a < packets)(lambda: e0(a))
        when((a >= 2) & (a < packets + 2) if not isinstance(a, int) else 2 <= a < packets + 2)(lambda: e1(a - 2))
        when((a >= 3) & (a < packets + 3) if not isinstance(a, int) else 3 <= a < packets + 3)(lambda: e2(a - 3))

    def ag_drain():
        if not COMM:
            return

        @pl.loop(0, packets)
        def _(p):
            four, three = agb.at[p, :, 0], agb.at[p, pl.ds(0, 3), 0]
            remote(four, four, ag_send.at[p], ag_p.at[p], partner).wait_send()
            remote(three, three, ag_relay.at[p], ag_p.at[p], partner).wait_send()

    def rs0(t):
        s = lax.rem(t, 4)
        pl.when(t >= 4)(lambda: pl.semaphore_wait(credit0, 1))
        remote(part.at[t, :, 1 - c], R0.at[s], s0.at[s], r0.at[s], partner).start()
        local(part.at[t, :, c], PB.at[s], lp.at[s]).start()

    def plus(out, *terms):
        total = terms[0][...].astype(F32)
        for term in terms[1:]:
            total += term[...].astype(F32)
        out[...] = total.astype(BF16)

    def firsts(s):
        return (
            (PB.at[s, XO, 0], C.at[s, 0], ss.at[s, 0], rc.at[s, 0], right),
            (PB.at[s, XO, 1], C.at[s, 1], ss.at[s, 1], rc.at[s, 1], left),
            (PB.at[s, XR, 1], F.at[s, 0], ss.at[s, 2], rf.at[s, 0], right),
            (PB.at[s, XL, 0], F.at[s, 1], ss.at[s, 3], rf.at[s, 1], left),
        )

    def seconds(s):
        return (
            (Q.at[s, 0], F.at[s, 2], ss.at[s, 4], rf.at[s, 2], right),
            (Q.at[s, 1], F.at[s, 3], ss.at[s, 5], rf.at[s, 3], left),
        )

    def rs1(t):
        s = lax.rem(t, 4)
        remote(part.at[t, :, 1 - c], R0.at[s], s0.at[s], r0.at[s], partner).wait_recv()
        local(part.at[t, :, c], PB.at[s], lp.at[s]).wait()

        @pl.when(t >= 4)
        def _():
            pl.semaphore_wait(credit_l, 1)
            pl.semaphore_wait(credit_r, 1)

        @pl.loop(0, 2 * chips)
        def _(b):
            y, h = b // 2, lax.rem(b, 2)
            plus(PB.at[s, y, h], PB.at[s, y, h], R0.at[s, y, h])

        pl.when(t + 4 < packets)(lambda: pl.semaphore_signal(credit0, 1, device_id=partner, device_id_type=MESH))
        for send in firsts(s):
            remote(*send).start()

    def rs2(t):
        s = lax.rem(t, 4)
        for send in firsts(s)[:2]:
            remote(*send).wait_recv()
        plus(Q.at[s, 0], PB.at[s, XR, 0], C.at[s, 0])
        plus(Q.at[s, 1], PB.at[s, XL, 1], C.at[s, 1])
        for send in seconds(s):
            remote(*send).start()

    def rs3(t):
        s, g = lax.rem(t, 4), lax.rem(t, 2)
        for send in firsts(s)[2:] + seconds(s):
            remote(*send).wait_recv()
        pl.when(t >= 2)(lambda: local(G.at[g], gout.at[t - 2], g_sem.at[g]).wait())
        plus(G.at[g, 0], PB.at[s, X, 0], F.at[s, 1], F.at[s, 2])
        plus(G.at[g, 1], PB.at[s, X, 1], F.at[s, 0], F.at[s, 3])
        local(G.at[g], gout.at[t], g_sem.at[g]).start()
        for send in firsts(s) + seconds(s):
            remote(*send).wait_send()
        remote(part.at[t, :, 1 - c], R0.at[s], s0.at[s], r0.at[s], partner).wait_send()

        @pl.when(t + 4 < packets)
        def _():
            pl.semaphore_signal(credit_r, 1, device_id=left, device_id_type=MESH)
            pl.semaphore_signal(credit_l, 1, device_id=right, device_id_type=MESH)

    def rs_tick(k):
        if not COMM:
            return
        pl.when((k >= 0) & (k < packets))(lambda: rs0(k))
        pl.when((k >= 1) & (k < packets + 1))(lambda: rs1(k - 1))
        pl.when((k >= 2) & (k < packets + 2))(lambda: rs2(k - 2))
        pl.when((k >= 3) & (k < packets + 3))(lambda: rs3(k - 3))

    def p_down(layer, j):
        return layer * per_layer + 3 * (j // 2)

    def p_gu(layer, j):
        return p_down(layer, j) + 1 + lax.rem(j, 2)

    def gu_load(layer, j, slot):
        return local(agb.at[p_gu(layer, j)], WGU.at[slot], w_sem.at[slot, 0])

    def down_load(layer, j, slot):
        return local(agb.at[p_down(layer, j), :, lax.rem(j, 2)], WD.at[slot], w_sem.at[slot, 1])

    def w_in(slot, which):
        return WGU[slot, :, :, which].reshape(d, CH)

    def w_out(slot, half):
        return WD[slot, :, half].reshape(CH, CH)

    def normed(src, dst):
        @pl.loop(0, tokens // 256)
        def _(b):
            rows = pl.ds(pl.multiple_of(b * 256, 256), 256)
            wide = src[rows, :].astype(F32)
            scale = lax.rsqrt(jnp.mean(wide * wide, -1, keepdims=True) + EPS)
            dst[rows, :] = (wide * scale).astype(BF16)

    def rows_of(r):
        return pl.ds(pl.multiple_of(r * BM, BM), BM)

    blocks = tokens // BM

    def by_hidden(slot, rows):
        return nt(DY[rows, : d // 2], w_out(slot, 0)) + nt(DY[rows, d // 2 :], w_out(slot, 1))

    def through(gate, up, dh, rows):
        dh = dh.astype(BF16).astype(F32)
        sig = jax.nn.sigmoid(gate)
        act = gate * sig
        HID[rows, :] = (act * up).astype(BF16)
        DU[rows, :] = (dh * act).astype(BF16)
        DG[rows, :] = (dh * up * (sig * (1 + gate * (1 - sig)))).astype(BF16)

    def part_out(t):
        return local(DWS, part.at[t], dw_sem.at[0])

    def part_down(t, j):
        return local(DWD, part.at[t, :, lax.rem(j, 2)], dw_sem.at[1])

    def gradients(A, t, t_down, j):
        for half in range(2):
            g = tn(HID[...], DY[:, half * CH : (half + 1) * CH])
            DWD[:, half] = g.astype(BF16).reshape(chips, R, CH)
        part_down(t_down, j).start()
        for b in range(d // 256):
            cols = slice(256 * b, 256 * b + 256)
            for which, by in ((0, DG), (1, DU)):
                g = tn(A[:, cols], by[...])
                DWS[b, :, which] = g.astype(BF16).reshape(2, R, CH)
        part_out(t).start()

    def unit_gu(k):
        return 3 * (k // 2) + lax.rem(k, 2)

    def unit_down(k):
        return 3 * (k // 2) + 2

    def settle(k):
        part_out(unit_gu(k)).wait()
        part_down(unit_down(k), k).wait()

    if COMM:
        barrier = pltpu.get_barrier_semaphore()
        for to in (left, right, partner):
            pl.semaphore_signal(barrier, 1, device_id=to, device_id_type=MESH)
        pl.semaphore_wait(barrier, 3)
    load_x, load_dy = local(x, H, in_sem.at[0]), local(dy, DY, in_sem.at[1])
    load_x.start()
    load_dy.start()
    ag_tick(0)
    ag_tick(1)
    load_x.wait()
    normed(H, A0)
    ACC[...] = jnp.zeros_like(ACC)
    load_dy.wait()
    ag_tick(2)

    def saved(b, slot, out):
        if out:
            return local(ST.at[slot], save.at[b], st_sem.at[slot])
        return local(save.at[b], ST.at[slot], st_sem.at[slot])

    @pl.loop(0, chunks)
    def _(i):
        slot = lax.rem(i, 2)
        p = p_gu(0, i)

        @pl.when(slot == 0)
        def _():
            ag_tick(p + 2)
            ready(p - 1)

        ag_tick(p + 3)
        ready(p)
        if COMPUTE:
            gu_load(0, i, slot).start()
            down_load(0, i, slot).start()
            gu_load(0, i, slot).wait()
            down_load(0, i, slot).wait()

            @pl.loop(0, blocks)
            def _(r):
                rows = rows_of(r)
                b = i * blocks + r
                ss_ = lax.rem(b, 2)
                a = A0[rows, :]
                gate = nn(a, w_in(slot, 0))
                up = nn(a, w_in(slot, 1))
                pl.when(b >= 2)(lambda: saved(b - 2, ss_, True).wait())
                ST[ss_, 0] = gate
                ST[ss_, 1] = up
                saved(b, ss_, True).start()
                hid = (gate * jax.nn.sigmoid(gate) * up).astype(BF16)
                for half in range(2):
                    cols = slice(half * CH, half * CH + CH)
                    ACC[rows, cols] += nn(hid, w_out(slot, half))

    last = chunks * blocks
    if COMPUTE:
        for b in (last - 2, last - 1):
            saved(b, b % 2, True).wait()
    ag_tick(per_layer + 3)
    if COMPUTE:
        @pl.loop(0, tokens // 256)
        def _(b):
            rows = pl.ds(pl.multiple_of(b * 256, 256), 256)
            h = (H[rows, :].astype(F32) + ACC[rows, :].astype(BF16).astype(F32)).astype(BF16)
            H[rows, :] = h
            wide = h.astype(F32)
            scale = lax.rsqrt(jnp.mean(wide * wide, -1, keepdims=True) + EPS)
            A1[rows, :] = (wide * scale).astype(BF16)
            ACC[rows, :] = jnp.zeros((256, d), F32)
    ag_tick(per_layer + 4)
    ready(per_layer)
    ready(per_layer + 1)
    if COMPUTE:
        gu_load(1, 0, 0).start()
        down_load(1, 0, 0).start()

    @pl.loop(0, chunks)
    def _(i):
        slot = lax.rem(i, 2)
        if COMPUTE:
            gu_load(1, i, slot).wait()
            down_load(1, i, slot).wait()
        ag_tick(per_layer + 5 + 2 * i)

        @pl.when(i + 1 < chunks)
        def _():
            p = p_gu(1, i + 1)
            pl.when(slot == 1)(lambda: ready(p - 1))
            ready(p)
            if COMPUTE:
                gu_load(1, i + 1, 1 - slot).start()
                down_load(1, i + 1, 1 - slot).start()

        if COMPUTE:
            @pl.loop(0, blocks)
            def _(r):
                rows = rows_of(r)
                a = A1[rows, :]
                through(nn(a, w_in(slot, 0)), nn(a, w_in(slot, 1)), by_hidden(slot, rows), rows)
                ACC[rows, :] += nt(DG[rows, :], w_in(slot, 0)) + nt(DU[rows, :], w_in(slot, 1))

            pl.when(i >= 1)(lambda: settle(i - 1))
        pl.when(i >= 1)(lambda: rs_tick(unit_gu(i - 1)))
        ag_tick(per_layer + 6 + 2 * i)
        if COMPUTE:
            gradients(A1, unit_gu(i), unit_down(i), i)
        pl.when((i >= 1) & (slot == 0))(lambda: rs_tick(unit_down(i - 1)))

    if COMPUTE:
        down_load(0, 0, 0).start()
        for b in range(2):
            saved(b, b, False).start()

        @pl.loop(0, tokens // 256)
        def _(b):
            rows = pl.ds(pl.multiple_of(b * 256, 256), 256)
            wide = H[rows, :].astype(F32)
            by = ACC[rows, :].astype(BF16).astype(F32)
            scale = lax.rsqrt(jnp.mean(wide * wide, -1, keepdims=True) + EPS)
            inner = jnp.mean(by * wide, -1, keepdims=True)
            back = (by * scale - wide * (scale * scale * scale * inner)).astype(BF16)
            DY[rows, :] = (DY[rows, :].astype(F32) + back.astype(F32)).astype(BF16)

    @pl.loop(0, chunks)
    def _(i):
        slot = lax.rem(i, 2)
        k = chunks + i
        if COMPUTE:
            down_load(0, i, slot).wait()
            pl.when(i + 1 < chunks)(lambda: down_load(0, i + 1, 1 - slot).start())

            @pl.loop(0, blocks)
            def _(r):
                rows = rows_of(r)
                b = i * blocks + r
                ss_ = lax.rem(b, 2)
                saved(b, ss_, False).wait()
                through(ST[ss_, 0], ST[ss_, 1], by_hidden(slot, rows), rows)
                pl.when(b + 2 < last)(lambda: saved(b + 2, ss_, False).start())

            settle(k - 1)
        rs_tick(unit_gu(k - 1))
        if COMPUTE:
            gradients(A0, unit_gu(k), unit_down(k), i)
        pl.when(slot == 0)(lambda: rs_tick(unit_down(k - 1)))

    if COMPUTE:
        settle(2 * chunks - 1)

    @pl.loop(packets - 2, packets + 3)
    def _(k):
        rs_tick(k)

    if COMM:
        for t in (packets - 2, packets - 1):
            local(G.at[t % 2], gout.at[t], g_sem.at[t % 2]).wait()
    ag_drain()


def gradients_of(mesh, x, dy, own):
    chips = mesh.shape["dp"] // 2
    packets = own.shape[0]
    tokens, d = x.shape
    layers = 2
    groups = packets // layers // 3
    unit = (2, R, CH)
    dma, reg = pltpu.SemaphoreType.DMA, pltpu.SemaphoreType.REGULAR
    V = pltpu.VMEM
    chunks, blocks = 2 * groups, tokens // BM
    hbm = pl.BlockSpec(memory_space=pltpu.HBM)
    flops = 2 * tokens * d * (CH * chunks) * 15
    return pl.pallas_call(
        functools.partial(kernel, chips, layers, groups),
        out_shape=(
            jax.ShapeDtypeStruct((packets, *unit), BF16),
            jax.ShapeDtypeStruct((packets, chips, 2, *unit), BF16),
            jax.ShapeDtypeStruct((packets, chips, 2, *unit), BF16),
            jax.ShapeDtypeStruct((chunks * blocks, 2, BM, CH), F32),
        ),
        in_specs=[hbm] * 3,
        out_specs=(hbm,) * 4,
        scratch_shapes=[
            V((tokens, d), BF16), V((tokens, d), BF16), V((tokens, d), BF16), V((tokens, d), BF16), V((tokens, d), F32),
            V((2, chips, 2, *unit), BF16), V((2, chips, *unit), BF16),
            V((tokens, CH), BF16), V((tokens, CH), BF16), V((tokens, CH), BF16),
            V((2, 2, BM, CH), F32), V((chips, 2, *unit), BF16), V((chips, *unit), BF16),
            V((4, chips, *unit), BF16), V((4, chips, *unit), BF16), V((4, *unit), BF16), V((4, 4, R, CH), BF16), V((4, *unit), BF16),
            V((2, *unit), BF16),
            dma((2,)), *[dma((packets,))] * 7, dma((2, 2)), dma((2,)), dma((2,)),
            dma((4,)), dma((4,)), dma((4,)), dma((4, 6)), dma((4, 2)), dma((4, 4)), dma((2,)), reg, reg, reg,
        ],
        compiler_params=pltpu.CompilerParams(collective_id=0, has_side_effects=True, vmem_limit_bytes=67043328),
        cost_estimate=pl.CostEstimate(flops=flops, bytes_accessed=300 << 20, transcendentals=0),
        name="step",
    )(x, dy, own)[0]


def adamw(w, m, v, g):
    m = 0.9 * m + 0.1 * g
    v = 0.95 * v + 0.05 * g * g
    step = m * lax.rsqrt(v + 1e-8) + 0.1 * w
    return (w - 0.02 * step).astype(jnp.bfloat16), m, v


def solution(mesh):
    chips = mesh.shape["dp"] // 2

    def step(x, dy, *arrays):
        weights, m, v = (arrays[i : i + 3] for i in (0, 3, 6))
        layers, _, ff = weights[0].shape
        d = weights[2].shape[2]
        groups = ff // (2 * chips) // R

        def spread(w):
            return w.reshape(layers, R, chips, 2, groups, R).transpose(0, 4, 3, 1, 2, 5).reshape(layers, groups, 2, R, CH)

        gu = jnp.stack([spread(weights[0]), spread(weights[1])], 3)
        down = weights[2].reshape(layers, groups, R, 2, CH).transpose(0, 1, 3, 2, 4)
        own = jnp.concatenate([down[:, :, None], gu], 2).reshape(-1, 2, R, CH)
        g = gradients_of(mesh, x[0], dy[0], own).reshape(layers, groups, 3, 2, R, CH)[::-1]

        def gathered(which):
            return g[:, :, :2, which].reshape(layers, groups, 2, R, chips, R).transpose(0, 3, 4, 2, 1, 5).reshape(layers, R, ff)

        g_down = g[:, :, 2].transpose(0, 1, 3, 2, 4).reshape(layers, groups * R, d)
        gradients = [one.astype(jnp.float32) for one in (gathered(0), gathered(1), g_down)]
        new = [adamw(w.astype(jnp.float32), m, v, g) for w, m, v, g in zip(weights, m, v, gradients, strict=True)]
        return tuple(one[which] for which in range(3) for one in new)

    states, cut = P(("rep", "dp"), None, None), P(None, "dp", None)
    return jax.shard_map(
        step,
        mesh=mesh,
        in_specs=(states, states) + (cut,) * 9,
        out_specs=(P("rep", "dp", None),) * 9,
        check_vma=False,
    )
```

```python
import functools

import jax
import jax.numpy as jnp
from jax import lax
from jax.experimental import pallas as pl
from jax.experimental.pallas import tpu as pltpu
from jax.sharding import PartitionSpec as P

NAMES = ("w_gate", "w_up", "w_down")
MESH = pl.DeviceIdType.MESH
F32, BF16 = jnp.float32, jnp.bfloat16
R = 128
CH = 512
BM = 512
EPS = 1e-6
OWN_SLOTS = 8
LEAD = 2
COMM = True
AG = True
RS = True
COMPUTE = True


def nn(a, b):
    return jnp.dot(a, b, preferred_element_type=F32)


def nt(a, b):
    return lax.dot_general(a, b, (((1,), (1,)), ((), ())), preferred_element_type=F32)


def tn(a, b):
    return lax.dot_general(a, b, (((0,), (0,)), ((), ())), preferred_element_type=F32)


def kernel(
    chips, layers, groups, x, dy, wg, wu, wd, gg, gu, gd, agb, part, save,
    A0, A1, H, DY, ACC, WGU, WD, HID, DG, DU, ST, DWS, DWD, R0, PB, C, F, Q, G, OWN,
    in_sem, own_sem, ag_send, ag_relay, ag_l, ag_r, ag_o, ag_p, ag_loc, w_sem, st_sem, dw_sem,
    s0, r0, lp, ss, rc, rf, g_sem, credit0, credit_l, credit_r,
):
    tokens, d = x.shape
    per_layer = 3 * groups
    packets = layers * per_layer
    chunks = 2 * groups
    me = lax.axis_index("dp")
    X, c = me // 2, lax.rem(me, 2)
    XR, XL, XO = lax.rem(X + 1, chips), lax.rem(X + chips - 1, chips), lax.rem(X + 2, chips)
    right, left, partner = {"dp": 2 * XR + c}, {"dp": 2 * XL + c}, {"dp": 2 * X + 1 - c}

    def remote(src, dst, send, recv, to):
        return pltpu.make_async_remote_copy(src_ref=src, dst_ref=dst, send_sem=send, recv_sem=recv, device_id=to, device_id_type=MESH)

    local = pltpu.make_async_copy

    def when(cond):
        if isinstance(cond, bool):
            return (lambda f: f()) if cond else (lambda f: None)
        return pl.when(cond)

    def place(t):
        rest = lax.rem(t, per_layer)
        return t // per_layer, rest // 3, lax.rem(rest, 3)

    def gu_cols(y, parity, q):
        return pl.ds(pl.multiple_of(((2 * y + parity) * groups + q) * R, R), R)

    def own_load(p):
        layer, q, k = place(p)
        s = lax.rem(p, OWN_SLOTS)

        @pl.when(k == 0)
        def _():
            for half in range(2):
                src = wd.at[layer, pl.ds(pl.multiple_of(q * R, R), R), half * CH : (half + 1) * CH]
                local(src, OWN.at[s, half], own_sem.at[s]).start()

        @pl.when(k > 0)
        def _():
            for which, w in enumerate((wg, wu)):
                for y in range(chips):
                    local(w.at[layer, :, gu_cols(y, k - 1, q)], OWN.at[s, which, :, y * R : (y + 1) * R], own_sem.at[s]).start()

    def sent(p):
        four = agb.at[p, :, 0]
        remote(four, four, ag_send.at[p], ag_p.at[p], partner).wait_send()

    def e0(p):
        s = lax.rem(p, OWN_SLOTS)
        local(agb.at[p, 0, 0], OWN.at[s], own_sem.at[s]).wait()
        for to, sem in ((right, ag_l), (left, ag_r), (partner, ag_p)):
            remote(OWN.at[s], agb.at[p, X, c], ag_send.at[p], sem.at[p], to).start()
        local(OWN.at[s], agb.at[p, X, c], ag_loc.at[p]).start()
        ahead = p + 2

        @pl.when(ahead < packets)
        def _():
            pl.when(ahead >= OWN_SLOTS)(lambda: sent(ahead - OWN_SLOTS))
            own_load(ahead)

    def e1(p):
        remote(agb.at[p, XL, c], agb.at[p, XL, c], ag_send.at[p], ag_l.at[p], right).wait_recv()
        remote(agb.at[p, XL, c, 0], agb.at[p, XL, c, 0], ag_send.at[p], ag_o.at[p], right).start()
        remote(agb.at[p, XL, c], agb.at[p, XL, c], ag_relay.at[p], ag_p.at[p], partner).start()
        remote(agb.at[p, XR, c], agb.at[p, XR, c], ag_send.at[p], ag_r.at[p], left).wait_recv()
        remote(agb.at[p, XR, c, 1], agb.at[p, XR, c, 1], ag_send.at[p], ag_o.at[p], left).start()
        remote(agb.at[p, XR, c], agb.at[p, XR, c], ag_relay.at[p], ag_p.at[p], partner).start()

    def e2(p):
        remote(agb.at[p, XO, c], agb.at[p, XO, c], ag_relay.at[p], ag_o.at[p], partner).wait_recv()
        remote(agb.at[p, XO, c], agb.at[p, XO, c], ag_relay.at[p], ag_p.at[p], partner).start()

    def ready(p):
        if not AG:
            return
        everyone = agb.at[p, :, 1 - c]
        remote(everyone, everyone, ag_relay.at[p], ag_p.at[p], partner).wait_recv()
        local(OWN.at[0], agb.at[p, X, c], ag_loc.at[p]).wait()

    def ag_tick(a):
        if not AG:
            return
        def at(k, do):
            when(0 <= k < packets if isinstance(k, int) else (k >= 0) & (k < packets))(lambda: do(k))

        at(a, e0)
        at(a - LEAD, e1)
        at(a - LEAD - 1, e2)

    def ag_drain():
        if not AG:
            return

        @pl.loop(0, packets)
        def _(p):
            three = agb.at[p, pl.ds(0, 3), 0]
            pl.when(p >= packets - OWN_SLOTS)(lambda: sent(p))
            remote(three, three, ag_relay.at[p], ag_p.at[p], partner).wait_send()

    def rs0(t):
        s = lax.rem(t, 4)
        pl.when(t >= 4)(lambda: pl.semaphore_wait(credit0, 1))
        remote(part.at[t, :, 1 - c], R0.at[s], s0.at[s], r0.at[s], partner).start()
        local(part.at[t, :, c], PB.at[s], lp.at[s]).start()

    def plus(out, *terms):
        total = terms[0][...].astype(F32)
        for term in terms[1:]:
            total += term[...].astype(F32)
        out[...] = total.astype(BF16)

    def firsts(s):
        return (
            (PB.at[s, XO, 0], C.at[s, 0], ss.at[s, 0], rc.at[s, 0], right),
            (PB.at[s, XO, 1], C.at[s, 1], ss.at[s, 1], rc.at[s, 1], left),
            (PB.at[s, XR, 1], F.at[s, 0], ss.at[s, 2], rf.at[s, 0], right),
            (PB.at[s, XL, 0], F.at[s, 1], ss.at[s, 3], rf.at[s, 1], left),
        )

    def seconds(s):
        return (
            (Q.at[s, 0], F.at[s, 2], ss.at[s, 4], rf.at[s, 2], right),
            (Q.at[s, 1], F.at[s, 3], ss.at[s, 5], rf.at[s, 3], left),
        )

    def rs1(t):
        s = lax.rem(t, 4)
        remote(part.at[t, :, 1 - c], R0.at[s], s0.at[s], r0.at[s], partner).wait_recv()
        local(part.at[t, :, c], PB.at[s], lp.at[s]).wait()

        @pl.when(t >= 4)
        def _():
            pl.semaphore_wait(credit_l, 1)
            pl.semaphore_wait(credit_r, 1)

        @pl.loop(0, 2 * chips)
        def _(b):
            y, h = b // 2, lax.rem(b, 2)
            plus(PB.at[s, y, h], PB.at[s, y, h], R0.at[s, y, h])

        pl.when(t + 4 < packets)(lambda: pl.semaphore_signal(credit0, 1, device_id=partner, device_id_type=MESH))
        for send in firsts(s):
            remote(*send).start()

    def rs2(t):
        s = lax.rem(t, 4)
        for send in firsts(s)[:2]:
            remote(*send).wait_recv()
        plus(Q.at[s, 0], PB.at[s, XR, 0], C.at[s, 0])
        plus(Q.at[s, 1], PB.at[s, XL, 1], C.at[s, 1])
        for send in seconds(s):
            remote(*send).start()

    def g_wait(g):
        local(G.at[g], agb.at[0, 0, 0], g_sem.at[g]).wait()

    def g_out(t, g):
        backward, q, k = place(t)
        layer = layers - 1 - backward

        @pl.when(k == 2)
        def _():
            for half in range(2):
                dst = gd.at[layer, pl.ds(pl.multiple_of(q * R, R), R), half * CH : (half + 1) * CH]
                local(G.at[g, half], dst, g_sem.at[g]).start()

        @pl.when(k < 2)
        def _():
            for which, out in enumerate((gg, gu)):
                for y in range(chips):
                    local(G.at[g, which, :, y * R : (y + 1) * R], out.at[layer, :, gu_cols(y, k, q)], g_sem.at[g]).start()

    def rs3(t):
        s, g = lax.rem(t, 4), lax.rem(t, 2)
        for send in firsts(s)[2:] + seconds(s):
            remote(*send).wait_recv()
        pl.when(t >= 2)(lambda: g_wait(g))
        plus(G.at[g, 0], PB.at[s, X, 0], F.at[s, 1], F.at[s, 2])
        plus(G.at[g, 1], PB.at[s, X, 1], F.at[s, 0], F.at[s, 3])
        g_out(t, g)
        for send in firsts(s) + seconds(s):
            remote(*send).wait_send()
        remote(part.at[t, :, 1 - c], R0.at[s], s0.at[s], r0.at[s], partner).wait_send()

        @pl.when(t + 4 < packets)
        def _():
            pl.semaphore_signal(credit_r, 1, device_id=left, device_id_type=MESH)
            pl.semaphore_signal(credit_l, 1, device_id=right, device_id_type=MESH)

    def rs_tick(k):
        if not RS:
            return
        pl.when((k >= 0) & (k < packets))(lambda: rs0(k))
        pl.when((k >= 1) & (k < packets + 1))(lambda: rs1(k - 1))
        pl.when((k >= 2) & (k < packets + 2))(lambda: rs2(k - 2))
        pl.when((k >= 3) & (k < packets + 3))(lambda: rs3(k - 3))

    def p_down(layer, j):
        return layer * per_layer + 3 * (j // 2)

    def p_gu(layer, j):
        return p_down(layer, j) + 1 + lax.rem(j, 2)

    def gu_load(layer, j, slot):
        return local(agb.at[p_gu(layer, j)], WGU.at[slot], w_sem.at[slot, 0])

    def down_load(layer, j, slot):
        return local(agb.at[p_down(layer, j), :, lax.rem(j, 2)], WD.at[slot], w_sem.at[slot, 1])

    def w_in(slot, which):
        return WGU[slot, :, :, which].reshape(d, CH)

    def w_out(slot, half):
        return WD[slot, :, half].reshape(CH, CH)

    def normed(src, dst):
        @pl.loop(0, tokens // 256)
        def _(b):
            rows = pl.ds(pl.multiple_of(b * 256, 256), 256)
            wide = src[rows, :].astype(F32)
            scale = lax.rsqrt(jnp.mean(wide * wide, -1, keepdims=True) + EPS)
            dst[rows, :] = (wide * scale).astype(BF16)

    def rows_of(r):
        return pl.ds(pl.multiple_of(r * BM, BM), BM)

    blocks = tokens // BM

    def by_hidden(slot, rows):
        return nt(DY[rows, : d // 2], w_out(slot, 0)) + nt(DY[rows, d // 2 :], w_out(slot, 1))

    def through(gate, up, dh, rows):
        dh = dh.astype(BF16).astype(F32)
        sig = jax.nn.sigmoid(gate)
        act = gate * sig
        HID[rows, :] = (act * up).astype(BF16)
        DU[rows, :] = (dh * act).astype(BF16)
        DG[rows, :] = (dh * up * (sig * (1 + gate * (1 - sig)))).astype(BF16)

    def part_out(t):
        return local(DWS, part.at[t], dw_sem.at[0])

    def part_down(t, j):
        return local(DWD, part.at[t, :, lax.rem(j, 2)], dw_sem.at[1])

    def gradients(A, t, t_down, j):
        for half in range(2):
            g = tn(HID[...], DY[:, half * CH : (half + 1) * CH])
            DWD[:, half] = g.astype(BF16).reshape(chips, R, CH)
        part_down(t_down, j).start()
        for b in range(d // 256):
            cols = slice(256 * b, 256 * b + 256)
            for which, by in ((0, DG), (1, DU)):
                g = tn(A[:, cols], by[...])
                DWS[b, :, which] = g.astype(BF16).reshape(2, R, CH)
        part_out(t).start()

    def unit_gu(k):
        return 3 * (k // 2) + lax.rem(k, 2)

    def unit_down(k):
        return 3 * (k // 2) + 2

    def settle(k):
        part_out(unit_gu(k)).wait()
        part_down(unit_down(k), k).wait()

    if COMM:
        barrier = pltpu.get_barrier_semaphore()
        for to in (left, right, partner):
            pl.semaphore_signal(barrier, 1, device_id=to, device_id_type=MESH)
        pl.semaphore_wait(barrier, 3)
    load_x, load_dy = local(x, H, in_sem.at[0]), local(dy, DY, in_sem.at[1])
    load_x.start()
    load_dy.start()
    if AG:
        own_load(0)
        own_load(1)
    ag_tick(0)
    ag_tick(1)
    load_x.wait()
    normed(H, A0)
    ACC[...] = jnp.zeros_like(ACC)
    load_dy.wait()
    for a in range(2, LEAD + 3):
        ag_tick(a)
    ready(0)
    ready(1)
    if COMPUTE:
        gu_load(0, 0, 0).start()
        down_load(0, 0, 0).start()

    def saved(b, slot, out):
        if out:
            return local(ST.at[slot], save.at[b], st_sem.at[slot])
        return local(save.at[b], ST.at[slot], st_sem.at[slot])

    def fetch(layer, j, slot):
        p = p_gu(layer, j)
        pl.when(lax.rem(j, 2) == 0)(lambda: ready(p - 1))
        ready(p)
        if COMPUTE:
            gu_load(layer, j, slot).start()
            down_load(layer, j, slot).start()

    @pl.loop(0, chunks)
    def _(i):
        slot = lax.rem(i, 2)
        following = i + 1
        p = per_layer * (following // chunks) + 3 * (lax.rem(following, chunks) // 2) + 1 + lax.rem(following, 2)
        if COMPUTE:
            gu_load(0, i, slot).wait()
            down_load(0, i, slot).wait()

        @pl.loop(0, blocks)
        def _(r):
            pl.when((r == 0) & (slot == 1))(lambda: ag_tick(p + LEAD))
            pl.when(r == 1)(lambda: ag_tick(p + LEAD + 1))
            pl.when((r == blocks - 1) & (following < chunks))(lambda: fetch(0, following, 1 - slot))
            if COMPUTE:
                rows = rows_of(r)
                b = i * blocks + r
                ss_ = lax.rem(b, 2)
                a = A0[rows, :]
                gate = nn(a, w_in(slot, 0))
                up = nn(a, w_in(slot, 1))
                pl.when(b >= 2)(lambda: saved(b - 2, ss_, True).wait())
                ST[ss_, 0] = gate
                ST[ss_, 1] = up
                saved(b, ss_, True).start()
                hid = (gate * jax.nn.sigmoid(gate) * up).astype(BF16)
                for half in range(2):
                    cols = slice(half * CH, half * CH + CH)
                    ACC[rows, cols] += nn(hid, w_out(slot, half))

    last = chunks * blocks
    if COMPUTE:
        for b in (last - 2, last - 1):
            saved(b, b % 2, True).wait()

        @pl.loop(0, tokens // 256)
        def _(b):
            rows = pl.ds(pl.multiple_of(b * 256, 256), 256)
            h = (H[rows, :].astype(F32) + ACC[rows, :].astype(BF16).astype(F32)).astype(BF16)
            H[rows, :] = h
            wide = h.astype(F32)
            scale = lax.rsqrt(jnp.mean(wide * wide, -1, keepdims=True) + EPS)
            A1[rows, :] = (wide * scale).astype(BF16)
            ACC[rows, :] = jnp.zeros((256, d), F32)
    fetch(1, jnp.int32(0), 0)

    @pl.loop(0, chunks)
    def _(i):
        slot = lax.rem(i, 2)
        if COMPUTE:
            gu_load(1, i, slot).wait()
            down_load(1, i, slot).wait()

        @pl.loop(0, blocks)
        def _(r):
            pl.when(r == 0)(lambda: ag_tick(per_layer + 3 + LEAD + 2 * i))
            pl.when(r == 2)(lambda: ag_tick(per_layer + 4 + LEAD + 2 * i))

            @pl.when((r == 1) & (i >= 1))
            def _():
                if COMPUTE:
                    settle(i - 1)
                rs_tick(unit_gu(i - 1))

            pl.when((r == 3) & (i >= 1) & (slot == 0))(lambda: rs_tick(unit_down(i - 1)))
            if COMPUTE:
                rows = rows_of(r)
                a = A1[rows, :]
                through(nn(a, w_in(slot, 0)), nn(a, w_in(slot, 1)), by_hidden(slot, rows), rows)
                ACC[rows, :] += nt(DG[rows, :], w_in(slot, 0)) + nt(DU[rows, :], w_in(slot, 1))

        pl.when(i + 1 < chunks)(lambda: fetch(1, i + 1, 1 - slot))
        if COMPUTE:
            gradients(A1, unit_gu(i), unit_down(i), i)

    if COMPUTE:
        down_load(0, 0, 0).start()
        for b in range(2):
            saved(b, b, False).start()

        @pl.loop(0, tokens // 256)
        def _(b):
            rows = pl.ds(pl.multiple_of(b * 256, 256), 256)
            wide = H[rows, :].astype(F32)
            by = ACC[rows, :].astype(BF16).astype(F32)
            scale = lax.rsqrt(jnp.mean(wide * wide, -1, keepdims=True) + EPS)
            inner = jnp.mean(by * wide, -1, keepdims=True)
            back = (by * scale - wide * (scale * scale * scale * inner)).astype(BF16)
            DY[rows, :] = (DY[rows, :].astype(F32) + back.astype(F32)).astype(BF16)

    @pl.loop(0, chunks)
    def _(i):
        slot = lax.rem(i, 2)
        k = chunks + i
        if COMPUTE:
            down_load(0, i, slot).wait()
            pl.when(i + 1 < chunks)(lambda: down_load(0, i + 1, 1 - slot).start())

        @pl.loop(0, blocks)
        def _(r):
            @pl.when(r == 1)
            def _():
                if COMPUTE:
                    settle(k - 1)
                rs_tick(unit_gu(k - 1))

            pl.when((r == 3) & (slot == 0))(lambda: rs_tick(unit_down(k - 1)))
            if COMPUTE:
                rows = rows_of(r)
                b = i * blocks + r
                ss_ = lax.rem(b, 2)
                saved(b, ss_, False).wait()
                through(ST[ss_, 0], ST[ss_, 1], by_hidden(slot, rows), rows)
                pl.when(b + 2 < last)(lambda: saved(b + 2, ss_, False).start())

        if COMPUTE:
            gradients(A0, unit_gu(k), unit_down(k), i)

    if COMPUTE:
        settle(2 * chunks - 1)

    @pl.loop(packets - 2, packets + 3)
    def _(k):
        rs_tick(k)

    if RS:
        for t in (packets - 2, packets - 1):
            g_wait(t % 2)
    ag_drain()


def gradients_of(mesh, x, dy, wg, wu, wd):
    chips = mesh.shape["dp"] // 2
    tokens, d = x.shape
    layers, hidden, _ = wd.shape
    groups = hidden // R
    packets = layers * 3 * groups
    unit = (2, R, CH)
    dma, reg = pltpu.SemaphoreType.DMA, pltpu.SemaphoreType.REGULAR
    V = pltpu.VMEM
    chunks, blocks = 2 * groups, tokens // BM
    hbm = pl.BlockSpec(memory_space=pltpu.HBM)
    flops = 2 * tokens * d * (CH * chunks) * 15
    return pl.pallas_call(
        functools.partial(kernel, chips, layers, groups),
        out_shape=(
            *(jax.ShapeDtypeStruct(w.shape, BF16) for w in (wg, wu, wd)),
            jax.ShapeDtypeStruct((packets, chips, 2, *unit), BF16),
            jax.ShapeDtypeStruct((packets, chips, 2, *unit), BF16),
            jax.ShapeDtypeStruct((chunks * blocks, 2, BM, CH), F32),
        ),
        in_specs=[hbm] * 5,
        out_specs=(hbm,) * 6,
        scratch_shapes=[
            V((tokens, d), BF16), V((tokens, d), BF16), V((tokens, d), BF16), V((tokens, d), BF16), V((tokens, d), F32),
            V((2, chips, 2, *unit), BF16), V((2, chips, *unit), BF16),
            V((tokens, CH), BF16), V((tokens, CH), BF16), V((tokens, CH), BF16),
            V((2, 2, BM, CH), F32), V((chips, 2, *unit), BF16), V((chips, *unit), BF16),
            V((4, chips, *unit), BF16), V((4, chips, *unit), BF16), V((4, *unit), BF16), V((4, 4, R, CH), BF16), V((4, *unit), BF16),
            V((2, *unit), BF16), V((OWN_SLOTS, *unit), BF16),
            dma((2,)), dma((OWN_SLOTS,)), *[dma((packets,))] * 7, dma((2, 2)), dma((2,)), dma((2,)),
            dma((4,)), dma((4,)), dma((4,)), dma((4, 6)), dma((4, 2)), dma((4, 4)), dma((2,)), reg, reg, reg,
        ],
        compiler_params=pltpu.CompilerParams(collective_id=0 if COMM else None, has_side_effects=True, vmem_limit_bytes=67043328),
        cost_estimate=pl.CostEstimate(flops=flops, bytes_accessed=300 << 20, transcendentals=0),
        name="step",
    )(x, dy, wg, wu, wd)[:3]


def adamw(w, m, v, g):
    m = 0.9 * m + 0.1 * g
    v = 0.95 * v + 0.05 * g * g
    step = m * lax.rsqrt(v + 1e-8) + 0.1 * w
    return (w - 0.02 * step).astype(jnp.bfloat16), m, v


def solution(mesh):
    def step(x, dy, *arrays):
        weights, m, v = (arrays[i : i + 3] for i in (0, 3, 6))
        gradients = [one.astype(jnp.float32) for one in gradients_of(mesh, x[0], dy[0], *weights)]
        new = [adamw(w.astype(jnp.float32), m, v, g) for w, m, v, g in zip(weights, m, v, gradients, strict=True)]
        return tuple(one[which] for which in range(3) for one in new)

    states, cut = P(("rep", "dp"), None, None), P(None, "dp", None)
    return jax.shard_map(
        step,
        mesh=mesh,
        in_specs=(states, states) + (cut,) * 9,
        out_specs=(P("rep", "dp", None),) * 9,
        check_vma=False,
    )
```

```python
import functools

import jax
import jax.numpy as jnp
from jax import lax
from jax.experimental import pallas as pl
from jax.experimental.pallas import tpu as pltpu
from jax.sharding import PartitionSpec as P

NAMES = ("w_gate", "w_up", "w_down")
MESH = pl.DeviceIdType.MESH
F32, BF16 = jnp.float32, jnp.bfloat16
R = 128
CH = 512
BM = 512
EPS = 1e-6
OWN_SLOTS = 10
LEAD = 2
COMM = True
AG = True
RS = True
COMPUTE = True


def nn(a, b):
    return jnp.dot(a, b, preferred_element_type=F32)


def nt(a, b):
    return lax.dot_general(a, b, (((1,), (1,)), ((), ())), preferred_element_type=F32)


def tn(a, b):
    return lax.dot_general(a, b, (((0,), (0,)), ((), ())), preferred_element_type=F32)


def kernel(
    chips, layers, groups, x, dy, wg, wu, wd, gg, gu, gd, agb, part, save,
    A0, A1, H, DY, ACC, WGU, WD, HID, DG, DU, ST, DWS, DWD, R0, PB, C, F, Q, G, OWN,
    in_sem, own_sem, ag_send, ag_relay, ag_l, ag_r, ag_o, ag_p, ag_loc, w_sem, st_sem, dw_sem,
    s0, r0, lp, ss, rc, rf, g_sem, credit0, credit_l, credit_r,
):
    tokens, d = x.shape
    per_layer = 3 * groups
    packets = layers * per_layer
    chunks = 2 * groups
    me = lax.axis_index("dp")
    X, c = me // 2, lax.rem(me, 2)
    XR, XL, XO = lax.rem(X + 1, chips), lax.rem(X + chips - 1, chips), lax.rem(X + 2, chips)
    right, left, partner = {"dp": 2 * XR + c}, {"dp": 2 * XL + c}, {"dp": 2 * X + 1 - c}

    def remote(src, dst, send, recv, to):
        return pltpu.make_async_remote_copy(src_ref=src, dst_ref=dst, send_sem=send, recv_sem=recv, device_id=to, device_id_type=MESH)

    local = pltpu.make_async_copy

    def when(cond):
        if isinstance(cond, bool):
            return (lambda f: f()) if cond else (lambda f: None)
        return pl.when(cond)

    def place(t):
        rest = lax.rem(t, per_layer)
        return t // per_layer, rest // 3, lax.rem(rest, 3)

    def gu_cols(y, parity, q):
        return pl.ds(pl.multiple_of(((2 * y + parity) * groups + q) * R, R), R)

    def own_load(p):
        layer, q, k = place(p)
        s = lax.rem(p, OWN_SLOTS)

        @pl.when(k == 0)
        def _():
            for half in range(2):
                src = wd.at[layer, pl.ds(pl.multiple_of(q * R, R), R), half * CH : (half + 1) * CH]
                local(src, OWN.at[s, half], own_sem.at[s]).start()

        @pl.when(k > 0)
        def _():
            for which, w in enumerate((wg, wu)):
                for y in range(chips):
                    local(w.at[layer, :, gu_cols(y, k - 1, q)], OWN.at[s, which, :, y * R : (y + 1) * R], own_sem.at[s]).start()

    def sent(p):
        four = agb.at[p, :, 0]
        remote(four, four, ag_send.at[p], ag_p.at[p], partner).wait_send()

    def e0(p):
        s = lax.rem(p, OWN_SLOTS)
        local(agb.at[p, 0, 0], OWN.at[s], own_sem.at[s]).wait()
        for to, sem in ((right, ag_l), (left, ag_r), (partner, ag_p)):
            remote(OWN.at[s], agb.at[p, X, c], ag_send.at[p], sem.at[p], to).start()
        local(OWN.at[s], agb.at[p, X, c], ag_loc.at[p]).start()
        ahead = p + 2

        @pl.when(ahead < packets)
        def _():
            pl.when(ahead >= OWN_SLOTS)(lambda: sent(ahead - OWN_SLOTS))
            own_load(ahead)

    def e1(p):
        remote(agb.at[p, XL, c], agb.at[p, XL, c], ag_send.at[p], ag_l.at[p], right).wait_recv()
        remote(agb.at[p, XL, c, 0], agb.at[p, XL, c, 0], ag_send.at[p], ag_o.at[p], right).start()
        remote(agb.at[p, XL, c], agb.at[p, XL, c], ag_relay.at[p], ag_p.at[p], partner).start()
        remote(agb.at[p, XR, c], agb.at[p, XR, c], ag_send.at[p], ag_r.at[p], left).wait_recv()
        remote(agb.at[p, XR, c, 1], agb.at[p, XR, c, 1], ag_send.at[p], ag_o.at[p], left).start()
        remote(agb.at[p, XR, c], agb.at[p, XR, c], ag_relay.at[p], ag_p.at[p], partner).start()

    def e2(p):
        remote(agb.at[p, XO, c], agb.at[p, XO, c], ag_relay.at[p], ag_o.at[p], partner).wait_recv()
        remote(agb.at[p, XO, c], agb.at[p, XO, c], ag_relay.at[p], ag_p.at[p], partner).start()

    def ready(p):
        if not AG:
            return
        everyone = agb.at[p, :, 1 - c]
        remote(everyone, everyone, ag_relay.at[p], ag_p.at[p], partner).wait_recv()
        local(OWN.at[0], agb.at[p, X, c], ag_loc.at[p]).wait()

    def ag_tick(a):
        if not AG:
            return
        def at(k, do):
            when(0 <= k < packets if isinstance(k, int) else (k >= 0) & (k < packets))(lambda: do(k))

        at(a, e0)
        at(a - LEAD, e1)
        at(a - LEAD - 1, e2)

    def ag_drain():
        if not AG:
            return

        @pl.loop(0, packets)
        def _(p):
            three = agb.at[p, pl.ds(0, 3), 0]
            pl.when(p >= packets - OWN_SLOTS)(lambda: sent(p))
            remote(three, three, ag_relay.at[p], ag_p.at[p], partner).wait_send()

    def rs0(t):
        s = lax.rem(t, 4)
        pl.when(t >= 4)(lambda: pl.semaphore_wait(credit0, 1))
        remote(part.at[t, :, 1 - c], R0.at[s], s0.at[s], r0.at[s], partner).start()
        local(part.at[t, :, c], PB.at[s], lp.at[s]).start()

    def plus(out, *terms):
        total = terms[0][...].astype(F32)
        for term in terms[1:]:
            total += term[...].astype(F32)
        out[...] = total.astype(BF16)

    def firsts(s):
        return (
            (PB.at[s, XO, 0], C.at[s, 0], ss.at[s, 0], rc.at[s, 0], right),
            (PB.at[s, XO, 1], C.at[s, 1], ss.at[s, 1], rc.at[s, 1], left),
            (PB.at[s, XR, 1], F.at[s, 0], ss.at[s, 2], rf.at[s, 0], right),
            (PB.at[s, XL, 0], F.at[s, 1], ss.at[s, 3], rf.at[s, 1], left),
        )

    def seconds(s):
        return (
            (Q.at[s, 0], F.at[s, 2], ss.at[s, 4], rf.at[s, 2], right),
            (Q.at[s, 1], F.at[s, 3], ss.at[s, 5], rf.at[s, 3], left),
        )

    def rs1(t):
        s = lax.rem(t, 4)
        remote(part.at[t, :, 1 - c], R0.at[s], s0.at[s], r0.at[s], partner).wait_recv()
        local(part.at[t, :, c], PB.at[s], lp.at[s]).wait()

        @pl.when(t >= 4)
        def _():
            pl.semaphore_wait(credit_l, 1)
            pl.semaphore_wait(credit_r, 1)

        @pl.loop(0, 2 * chips)
        def _(b):
            y, h = b // 2, lax.rem(b, 2)
            plus(PB.at[s, y, h], PB.at[s, y, h], R0.at[s, y, h])

        pl.when(t + 4 < packets)(lambda: pl.semaphore_signal(credit0, 1, device_id=partner, device_id_type=MESH))
        for send in firsts(s):
            remote(*send).start()

    def rs2(t):
        s = lax.rem(t, 4)
        for send in firsts(s)[:2]:
            remote(*send).wait_recv()
        plus(Q.at[s, 0], PB.at[s, XR, 0], C.at[s, 0])
        plus(Q.at[s, 1], PB.at[s, XL, 1], C.at[s, 1])
        for send in seconds(s):
            remote(*send).start()

    def g_wait(g):
        local(G.at[g], agb.at[0, 0, 0], g_sem.at[g]).wait()

    def g_out(t, g):
        backward, q, k = place(t)
        layer = layers - 1 - backward

        @pl.when(k == 1)
        def _():
            for half in range(2):
                dst = gd.at[layer, pl.ds(pl.multiple_of(q * R, R), R), half * CH : (half + 1) * CH]
                local(G.at[g, half], dst, g_sem.at[g]).start()

        @pl.when(k != 1)
        def _():
            for which, out in enumerate((gg, gu)):
                for y in range(chips):
                    local(G.at[g, which, :, y * R : (y + 1) * R], out.at[layer, :, gu_cols(y, k // 2, q)], g_sem.at[g]).start()

    def rs3(t):
        s, g = lax.rem(t, 4), lax.rem(t, 2)
        for send in firsts(s)[2:] + seconds(s):
            remote(*send).wait_recv()
        pl.when(t >= 2)(lambda: g_wait(g))
        plus(G.at[g, 0], PB.at[s, X, 0], F.at[s, 1], F.at[s, 2])
        plus(G.at[g, 1], PB.at[s, X, 1], F.at[s, 0], F.at[s, 3])
        g_out(t, g)
        for send in firsts(s) + seconds(s):
            remote(*send).wait_send()
        remote(part.at[t, :, 1 - c], R0.at[s], s0.at[s], r0.at[s], partner).wait_send()

        @pl.when(t + 4 < packets)
        def _():
            pl.semaphore_signal(credit_r, 1, device_id=left, device_id_type=MESH)
            pl.semaphore_signal(credit_l, 1, device_id=right, device_id_type=MESH)

    def rs_rest(k):
        if not RS:
            return
        pl.when((k >= 1) & (k < packets + 1))(lambda: rs1(k - 1))
        pl.when((k >= 2) & (k < packets + 2))(lambda: rs2(k - 2))
        pl.when((k >= 3) & (k < packets + 3))(lambda: rs3(k - 3))

    def rs_tick(k):
        if not RS:
            return
        pl.when(k < packets)(lambda: rs0(k))
        rs_rest(k)

    def p_down(layer, j):
        return layer * per_layer + 3 * (j // 2)

    def p_gu(layer, j):
        return p_down(layer, j) + 1 + lax.rem(j, 2)

    def gu_load(layer, j, slot):
        return local(agb.at[p_gu(layer, j)], WGU.at[slot], w_sem.at[slot, 0])

    def down_load(layer, j, slot):
        return local(agb.at[p_down(layer, j), :, lax.rem(j, 2)], WD.at[slot], w_sem.at[slot, 1])

    def w_in(slot, which):
        return WGU[slot, :, :, which].reshape(d, CH)

    def w_out(slot, half):
        return WD[slot, :, half].reshape(CH, CH)

    def normed(src, dst):
        @pl.loop(0, tokens // 256)
        def _(b):
            rows = pl.ds(pl.multiple_of(b * 256, 256), 256)
            wide = src[rows, :].astype(F32)
            scale = lax.rsqrt(jnp.mean(wide * wide, -1, keepdims=True) + EPS)
            dst[rows, :] = (wide * scale).astype(BF16)

    def rows_of(r):
        return pl.ds(pl.multiple_of(r * BM, BM), BM)

    blocks = tokens // BM

    def by_hidden(slot, rows):
        return nt(DY[rows, : d // 2], w_out(slot, 0)) + nt(DY[rows, d // 2 :], w_out(slot, 1))

    def through(gate, up, dh, rows):
        dh = dh.astype(BF16).astype(F32)
        sig = jax.nn.sigmoid(gate)
        act = gate * sig
        HID[rows, :] = (act * up).astype(BF16)
        DU[rows, :] = (dh * act).astype(BF16)
        DG[rows, :] = (dh * up * (sig * (1 + gate * (1 - sig)))).astype(BF16)

    def part_out(t):
        return local(DWS, part.at[t], dw_sem.at[0])

    def part_down(t, j):
        return local(DWD, part.at[t, :, lax.rem(j, 2)], dw_sem.at[1])

    def gradients(A, t, t_down, j):
        for half in range(2):
            g = tn(HID[...], DY[:, half * CH : (half + 1) * CH])
            DWD[:, half] = g.astype(BF16).reshape(chips, R, CH)
        part_down(t_down, j).start()
        for b in range(d // 256):
            if b == 1:
                @pl.when(lax.rem(j, 2) == 1)
                def _():
                    part_down(t_down, j).wait()
                    if RS:
                        rs0(t_down)
                    pl.when(t_down < packets - 2)(lambda: rs_rest(t_down))

            if b == 3:
                pl.when(t == packets - 1)(lambda: rs_rest(t))
            cols = slice(256 * b, 256 * b + 256)
            for which, by in ((0, DG), (1, DU)):
                g = tn(A[:, cols], by[...])
                DWS[b, :, which] = g.astype(BF16).reshape(2, R, CH)
        part_out(t).start()

    def unit_gu(k):
        return 3 * (k // 2) + 2 * lax.rem(k, 2)

    def unit_down(k):
        return 3 * (k // 2) + 1

    def settle(k):
        part_out(unit_gu(k)).wait()
        pl.when(lax.rem(k, 2) == 0)(lambda: part_down(unit_down(k), k).wait())

    if COMM:
        barrier = pltpu.get_barrier_semaphore()
        for to in (left, right, partner):
            pl.semaphore_signal(barrier, 1, device_id=to, device_id_type=MESH)
        pl.semaphore_wait(barrier, 3)
    load_x, load_dy = local(x, H, in_sem.at[0]), local(dy, DY, in_sem.at[1])
    load_x.start()
    load_dy.start()
    if AG:
        own_load(0)
        own_load(1)
    ag_tick(0)
    ag_tick(1)
    load_x.wait()
    normed(H, A0)
    ACC[...] = jnp.zeros_like(ACC)
    load_dy.wait()
    for a in range(2, LEAD + 3):
        ag_tick(a)
    ready(0)
    ready(1)
    if COMPUTE:
        gu_load(0, 0, 0).start()
        down_load(0, 0, 0).start()

    def saved(b, slot, out):
        if out:
            return local(ST.at[slot], save.at[b], st_sem.at[slot])
        return local(save.at[b], ST.at[slot], st_sem.at[slot])

    def fetch(layer, j, slot):
        p = p_gu(layer, j)
        pl.when(lax.rem(j, 2) == 0)(lambda: ready(p - 1))
        ready(p)
        if COMPUTE:
            gu_load(layer, j, slot).start()
            down_load(layer, j, slot).start()

    @pl.loop(0, chunks)
    def _(i):
        slot = lax.rem(i, 2)
        following = i + 1
        p = per_layer * (following // chunks) + 3 * (lax.rem(following, chunks) // 2) + 1 + lax.rem(following, 2)
        if COMPUTE:
            gu_load(0, i, slot).wait()
            down_load(0, i, slot).wait()

        @pl.loop(0, blocks)
        def _(r):
            pl.when((r == 0) & (slot == 1))(lambda: ag_tick(p + LEAD))
            pl.when(r == 1)(lambda: ag_tick(p + LEAD + 1))
            pl.when((r == blocks - 1) & (following < chunks))(lambda: fetch(0, following, 1 - slot))
            if COMPUTE:
                rows = rows_of(r)
                b = i * blocks + r
                ss_ = lax.rem(b, 2)
                a = A0[rows, :]
                gate = nn(a, w_in(slot, 0))
                up = nn(a, w_in(slot, 1))
                pl.when(b >= 2)(lambda: saved(b - 2, ss_, True).wait())
                ST[ss_, 0] = gate
                ST[ss_, 1] = up
                saved(b, ss_, True).start()
                hid = (gate * jax.nn.sigmoid(gate) * up).astype(BF16)
                for half in range(2):
                    cols = slice(half * CH, half * CH + CH)
                    ACC[rows, cols] += nn(hid, w_out(slot, half))

    last = chunks * blocks
    if COMPUTE:
        for b in (last - 2, last - 1):
            saved(b, b % 2, True).wait()

        @pl.loop(0, tokens // 256)
        def _(b):
            rows = pl.ds(pl.multiple_of(b * 256, 256), 256)
            h = (H[rows, :].astype(F32) + ACC[rows, :].astype(BF16).astype(F32)).astype(BF16)
            H[rows, :] = h
            wide = h.astype(F32)
            scale = lax.rsqrt(jnp.mean(wide * wide, -1, keepdims=True) + EPS)
            A1[rows, :] = (wide * scale).astype(BF16)
            ACC[rows, :] = jnp.zeros((256, d), F32)
    fetch(1, jnp.int32(0), 0)

    @pl.loop(0, chunks)
    def _(i):
        slot = lax.rem(i, 2)
        if COMPUTE:
            gu_load(1, i, slot).wait()
            down_load(1, i, slot).wait()

        @pl.loop(0, blocks)
        def _(r):
            first = per_layer + 3 + LEAD
            early = i < 2
            pl.when(early & (r != 1))(lambda: ag_tick(first + 3 * i + jnp.maximum(r - 1, 0)))
            pl.when((i >= 2) & (r == 0))(lambda: ag_tick(first + 4 + i))

            @pl.when((r == 1) & (i >= 1))
            def _():
                if COMPUTE:
                    settle(i - 1)
                rs_tick(unit_gu(i - 1))

            if COMPUTE:
                rows = rows_of(r)
                a = A1[rows, :]
                through(nn(a, w_in(slot, 0)), nn(a, w_in(slot, 1)), by_hidden(slot, rows), rows)
                ACC[rows, :] += nt(DG[rows, :], w_in(slot, 0)) + nt(DU[rows, :], w_in(slot, 1))

        pl.when(i + 1 < chunks)(lambda: fetch(1, i + 1, 1 - slot))
        if COMPUTE:
            gradients(A1, unit_gu(i), unit_down(i), i)

    if COMPUTE:
        down_load(0, 0, 0).start()
        for b in range(2):
            saved(b, b, False).start()

        @pl.loop(0, tokens // 256)
        def _(b):
            rows = pl.ds(pl.multiple_of(b * 256, 256), 256)
            wide = H[rows, :].astype(F32)
            by = ACC[rows, :].astype(BF16).astype(F32)
            scale = lax.rsqrt(jnp.mean(wide * wide, -1, keepdims=True) + EPS)
            inner = jnp.mean(by * wide, -1, keepdims=True)
            back = (by * scale - wide * (scale * scale * scale * inner)).astype(BF16)
            DY[rows, :] = (DY[rows, :].astype(F32) + back.astype(F32)).astype(BF16)

    @pl.loop(0, chunks)
    def _(i):
        slot = lax.rem(i, 2)
        k = chunks + i
        if COMPUTE:
            down_load(0, i, slot).wait()
            pl.when(i + 1 < chunks)(lambda: down_load(0, i + 1, 1 - slot).start())

        @pl.loop(0, blocks)
        def _(r):
            @pl.when(r == 1)
            def _():
                if COMPUTE:
                    settle(k - 1)
                rs_tick(unit_gu(k - 1))

            pl.when((r == 3) & (i == chunks - 1))(lambda: rs_rest(unit_gu(k - 1) + 1))
            if COMPUTE:
                rows = rows_of(r)
                b = i * blocks + r
                ss_ = lax.rem(b, 2)
                saved(b, ss_, False).wait()
                through(ST[ss_, 0], ST[ss_, 1], by_hidden(slot, rows), rows)
                pl.when(b + 2 < last)(lambda: saved(b + 2, ss_, False).start())

        if COMPUTE:
            gradients(A0, unit_gu(k), unit_down(k), i)

    if COMPUTE:
        settle(jnp.int32(2 * chunks - 1))
    if RS:
        rs0(jnp.int32(packets - 1))

        @pl.loop(packets, packets + 3)
        def _(k):
            rs_rest(k)

    if RS:
        for t in (packets - 2, packets - 1):
            g_wait(t % 2)
    ag_drain()


def gradients_of(mesh, x, dy, wg, wu, wd):
    chips = mesh.shape["dp"] // 2
    tokens, d = x.shape
    layers, hidden, _ = wd.shape
    groups = hidden // R
    packets = layers * 3 * groups
    unit = (2, R, CH)
    dma, reg = pltpu.SemaphoreType.DMA, pltpu.SemaphoreType.REGULAR
    V = pltpu.VMEM
    chunks, blocks = 2 * groups, tokens // BM
    hbm = pl.BlockSpec(memory_space=pltpu.HBM)
    flops = 2 * tokens * d * (CH * chunks) * 15
    return pl.pallas_call(
        functools.partial(kernel, chips, layers, groups),
        out_shape=(
            *(jax.ShapeDtypeStruct(w.shape, BF16) for w in (wg, wu, wd)),
            jax.ShapeDtypeStruct((packets, chips, 2, *unit), BF16),
            jax.ShapeDtypeStruct((packets, chips, 2, *unit), BF16),
            jax.ShapeDtypeStruct((chunks * blocks, 2, BM, CH), F32),
        ),
        in_specs=[hbm] * 5,
        out_specs=(hbm,) * 6,
        scratch_shapes=[
            V((tokens, d), BF16), V((tokens, d), BF16), V((tokens, d), BF16), V((tokens, d), BF16), V((tokens, d), F32),
            V((2, chips, 2, *unit), BF16), V((2, chips, *unit), BF16),
            V((tokens, CH), BF16), V((tokens, CH), BF16), V((tokens, CH), BF16),
            V((2, 2, BM, CH), F32), V((chips, 2, *unit), BF16), V((chips, *unit), BF16),
            V((4, chips, *unit), BF16), V((4, chips, *unit), BF16), V((4, *unit), BF16), V((4, 4, R, CH), BF16), V((4, *unit), BF16),
            V((2, *unit), BF16), V((OWN_SLOTS, *unit), BF16),
            dma((2,)), dma((OWN_SLOTS,)), *[dma((packets,))] * 7, dma((2, 2)), dma((2,)), dma((2,)),
            dma((4,)), dma((4,)), dma((4,)), dma((4, 6)), dma((4, 2)), dma((4, 4)), dma((2,)), reg, reg, reg,
        ],
        compiler_params=pltpu.CompilerParams(collective_id=0 if COMM else None, has_side_effects=True, vmem_limit_bytes=67043328),
        cost_estimate=pl.CostEstimate(flops=flops, bytes_accessed=300 << 20, transcendentals=0),
        name="step",
    )(x, dy, wg, wu, wd)[:3]


def adamw(w, m, v, g):
    m = 0.9 * m + 0.1 * g
    v = 0.95 * v + 0.05 * g * g
    step = m * lax.rsqrt(v + 1e-8) + 0.1 * w
    return (w - 0.02 * step).astype(jnp.bfloat16), m, v


def solution(mesh):
    def step(x, dy, *arrays):
        weights, m, v = (arrays[i : i + 3] for i in (0, 3, 6))
        gradients = [one.astype(jnp.float32) for one in gradients_of(mesh, x[0], dy[0], *weights)]
        new = [adamw(w.astype(jnp.float32), m, v, g) for w, m, v, g in zip(weights, m, v, gradients, strict=True)]
        return tuple(one[which] for which in range(3) for one in new)

    states, cut = P(("rep", "dp"), None, None), P(None, "dp", None)
    return jax.shard_map(
        step,
        mesh=mesh,
        in_specs=(states, states) + (cut,) * 9,
        out_specs=(P("rep", "dp", None),) * 9,
        check_vma=False,
    )
```
